32 devices in a mesh: row: 2 (over x), col: 16 (over z, y, core).
Axes of the slice: x: 2, y: 2, z: 4, core: 2. Of those that a mesh axis runs over, the one named last changes fastest.
Arguments:
- ld_matrix: bfloat16 [32768, 32768], P('row', 'col'), may hold values from -0.23925781 to 0.23925781
- factor: float32 [32768, 256], P(('row', 'col')), may hold values from -0.24 to 0.24
- diag_values: bfloat16 [32768], P('col'), may hold values from 0.5 to 4
Outputs:
- factor_grad: float32 [32768, 256], P(('row', 'col'))
The draws below stay inside these ranges and needn't reach their ends.
All inputs are finite; a program needn't handle non-finite values.
Results may differ from the reference program's by a relative error of at most 0.003.
Values may be sent and summed in bfloat16 or wider, within the bound.
A program may use at most 128 MiB of HBM per device.

```python
import math
import jax
import jax.numpy as jnp
from jax import lax

M = 32768
K = 256


def strengthened(values, stream_key, source, target, shards_of, factor):
    owner, partner = [(jnp.arange(values.shape[axis_at]) // (values.shape[axis_at] // shards_of)).reshape([-1 if axis == axis_at else 1 for axis in range(values.ndim)]) for axis_at in (source, target)]
    chosen = jax.random.permutation(stream_key, shards_of)[partner]
    strong = (owner == chosen) | (owner == (partner + shards_of // 2) % shards_of)
    return jnp.where(strong, factor * values, values)


def block_levels(rng, extent, split, smallest, high):
    def one(dim, parts):
        steps = jax.random.uniform(jax.random.fold_in(jax.random.fold_in(rng, 6), dim), (parts,), jnp.float32, smallest / len(split), high / len(split))
        return jnp.repeat(jnp.exp(steps), extent[dim] // parts).reshape((-1,) + (1,) * (len(extent) - dim - 1))

    level = one(*split[0])
    for cut in split[1:]:
        level = level * one(*cut)
    return level


def normal_values(stream_key, extent, deviation, reach, shards=(), kind=jnp.bfloat16):
    gain = block_levels(stream_key, extent, shards, -0.22, 0.18) if shards else 1.0
    entries = jax.random.normal(stream_key, extent, jnp.float32) * deviation * gain
    return jnp.minimum(jnp.maximum(entries, -reach), reach).astype(kind)


def heavy_noise(own_key, extent, width, most, split, heavy, held_as=jnp.bfloat16):
    drawn = width * jax.random.normal(own_key, extent, jnp.float32)
    if split:
        drawn = drawn * block_levels(own_key, extent, split, -0.22, 0.18)
    return jnp.clip(strengthened(drawn, jax.random.fold_in(own_key, 3), *heavy), -most, most).astype(held_as)


def setup_inputs(seed: int = 0) -> dict:
    key_list = jax.random.split(jax.random.key(seed), 4)
    return {
        "ld_matrix": heavy_noise(key_list[0], (M, M), 0.03, 0.23925781, ((0, 2), (1, 16)), (1, 0, 16, 2.0)),
        "factor": normal_values(key_list[1], (M, K), 0.03, 0.24, ((0, 32),), jnp.float32),
        "diag_values": jnp.clip(jnp.exp(math.log(4.0) - 2.0794415 * jax.random.uniform(key_list[2], (M,), jnp.float32) ** block_levels(key_list[2], (M,), ((0, 16),), -0.2, 0.2)), 0.5, 4.0).astype(jnp.bfloat16),
    }


def reference(ld_matrix, factor, diag_values):
    factor_low = factor.astype(jnp.bfloat16)
    height = min(1024, M)
    count = M // height
    ld_blocks = ld_matrix.reshape(count, height, M)
    diag_full = diag_values.astype(jnp.float32)
    columns = jnp.arange(M, dtype=jnp.int32)

    def one_block(inputs):
        index, ld_block = inputs
        start = (index * height).astype(jnp.int32)
        left = lax.dynamic_slice_in_dim(factor_low, start, height, 0)
        model_part = jnp.dot(left, factor_low.T, preferred_element_type=jnp.float32)
        row_ids = start + jnp.arange(height, dtype=jnp.int32)
        ondiag = row_ids[:, None] == columns[None, :]
        extra = jnp.where(ondiag, diag_full[None, :], jnp.float32(0.0))
        misfit = (model_part + extra - ld_block.astype(jnp.float32)).astype(jnp.bfloat16)
        return 4.0 * jnp.dot(misfit, factor_low, preferred_element_type=jnp.float32)

    result = lax.map(one_block, (jnp.arange(count, dtype=jnp.int32), ld_blocks))
    return result.reshape(M, K)
```

```python
import jax
import jax.numpy as jnp
from jax import lax
from jax.sharding import PartitionSpec as P


def local(ld_matrix, factor, diag_values):
    n_row, n_col = lax.axis_size("row"), lax.axis_size("col")
    row_index, col_index = lax.axis_index("row"), lax.axis_index("col")
    factor_low = factor.astype(jnp.bfloat16)
    own, rank = factor.shape
    width = ld_matrix.shape[1]
    panel = jnp.zeros((width, rank), jnp.bfloat16)
    for k in range(n_row):
        pairs = [
            (n_row * c + (r + k) % n_row, r * n_col + c)
            for r in range(n_row)
            for c in range(n_col)
        ]
        piece = lax.ppermute(factor_low, ("row", "col"), pairs)
        at = lax.rem(row_index + k, n_row) * own
        panel = lax.dynamic_update_slice_in_dim(panel, piece, at, 0)
    gram = lax.dot_general(
        factor_low, factor_low, (((0,), (0,)), ((), ())), preferred_element_type=jnp.float32
    )
    gram = lax.psum(gram, ("row", "col"))
    part = jnp.dot(ld_matrix, panel, preferred_element_type=jnp.float32)
    per_row = n_col // n_row
    first = col_index % per_row * width
    scale = jnp.where(row_index == col_index // per_row, diag_values, 0).astype(jnp.float32)
    slab = lax.dynamic_slice_in_dim(part, first, width, 0)
    slab = slab - scale[:, None] * panel.astype(jnp.float32)
    part = lax.dynamic_update_slice_in_dim(part, slab, first, 0).astype(jnp.bfloat16)
    total = lax.psum_scatter(part, "col", scatter_dimension=0, tiled=True)
    model = jnp.dot(factor_low, gram, precision=lax.Precision.HIGHEST, preferred_element_type=jnp.float32)
    return 4.0 * (model - total.astype(jnp.float32))


def solution(mesh):
    in_specs = (P("row", "col"), P(("row", "col"), None), P("col"))
    out_specs = P(("row", "col"), None)
    return jax.shard_map(local, mesh=mesh, in_specs=in_specs, out_specs=out_specs, check_vma=False)
```
